8 devices in a mesh: dp: 1 (over z), tp: 8 (over y, x, core).
Axes of the slice: x: 2, y: 2, z: 1, core: 2. Of those that a mesh axis runs over, the one named last changes fastest.
Arguments:
- x: bfloat16 [3072, 5120], P(('dp', 'tp'))
- dy: bfloat16 [3072, 5120], P(('dp', 'tp'))
- wg: bfloat16 [5120, 14336], P(None, 'tp')
- wu: bfloat16 [5120, 14336], P(None, 'tp')
- wd: bfloat16 [14336, 5120], P('tp')
- ug: bfloat16 [3072, 14336], P('dp', 'tp')
- uu: bfloat16 [3072, 14336], P('dp', 'tp')
Outputs:
- output 1: bfloat16 [3072, 5120], P(('dp', 'tp'))
- output 2: float32 [5120, 14336], P('dp', 'tp')
- output 3: float32 [5120, 14336], P('dp', 'tp')
- output 4: float32 [14336, 5120], P(('dp', 'tp'))
All inputs are finite; a program needn't handle non-finite values.
Results may differ from the reference program's by a relative error of at most 0.0116402.
Values are sent between devices in bfloat16 or wider.
A program may use at most 1 GiB of HBM per device.

```python
import jax
import jax.numpy as jnp

T = 3072
H = 5120
F = 14336


def setup_inputs(seed: int = 0, part: int = 0) -> dict:
    key = jax.random.key(seed)
    k_shared, k_part = jax.random.split(key)
    kg, ku, kd = jax.random.split(k_shared, 3)
    kx, kdy, kug, kuu = jax.random.split(jax.random.fold_in(k_part, part), 4)
    wg = (jax.random.normal(kg, (H, F), jnp.float32) * H ** -0.5).astype(jnp.bfloat16)
    wu = (jax.random.normal(ku, (H, F), jnp.float32) * H ** -0.5).astype(jnp.bfloat16)
    wd = (jax.random.normal(kd, (F, H), jnp.float32) * F ** -0.5).astype(jnp.bfloat16)
    x = jax.random.normal(kx, (T, H), jnp.float32).astype(jnp.bfloat16)
    dy = jax.random.normal(kdy, (T, H), jnp.float32).astype(jnp.bfloat16)
    ug = jax.random.normal(kug, (T, F), jnp.float32).astype(jnp.bfloat16)
    uu = jax.random.normal(kuu, (T, F), jnp.float32).astype(jnp.bfloat16)
    return {"x": x, "dy": dy, "wg": wg, "wu": wu, "wd": wd, "ug": ug, "uu": uu}


def reference(x, dy, wg, wu, wd, ug, uu):
    ug32 = ug.astype(jnp.float32)
    uu32 = uu.astype(jnp.float32)
    s = jax.nn.sigmoid(ug32)
    a = ug32 * s
    z = (a * uu32).astype(jnp.bfloat16)
    dwd = jnp.dot(z.T, dy, preferred_element_type=jnp.float32)
    g = jnp.dot(dy, wd.T, preferred_element_type=jnp.float32)
    duu = (g * a).astype(jnp.bfloat16)
    dug = (g * uu32 * s * (1.0 + ug32 * (1.0 - s))).astype(jnp.bfloat16)
    p = jnp.dot(dug, wg.T, preferred_element_type=jnp.float32) + jnp.dot(duu, wu.T, preferred_element_type=jnp.float32)
    dx = p.astype(jnp.bfloat16)
    dwg = jnp.dot(x.T, dug, preferred_element_type=jnp.float32)
    dwu = jnp.dot(x.T, duu, preferred_element_type=jnp.float32)
    return (dx, dwg, dwu, dwd)
```

```python
import functools

import jax
import jax.numpy as jnp
from jax import lax
from jax.experimental import pallas as pl
from jax.experimental.pallas import tpu as pltpu
from jax.sharding import PartitionSpec as P


BF16 = jnp.bfloat16
F32 = jnp.float32
VMEM_LIMIT = 60 * 1024 * 1024
ANY = pl.BlockSpec(memory_space=pl.ANY)
NT = (((1,), (1,)), ((), ()))
TN = (((0,), (0,)), ((), ()))


def params():
    return pltpu.CompilerParams(vmem_limit_bytes=VMEM_LIMIT)


def cost(m, k, n, nbytes):
    return pl.CostEstimate(flops=2 * m * k * n, bytes_accessed=nbytes, transcendentals=0)


def gp_chunk(dys, wd, ug, uu, wg, wu, places):
    f, h = wd.shape
    total = sum(d.shape[0] for d in dys)
    shard = ug.shape[0] // 8
    half = total // 2
    bg, bp = 512, 512
    gsteps, psteps = f // bg, h // bp
    rest = f - gsteps * bg
    wide = (gsteps + 1) * bg
    nd, npc = len(dys), len(places)

    def kernel(*refs):
        dy_refs = refs[:nd]
        wd_ref, ug_ref, uu_ref, wg_ref, wu_ref = refs[nd : nd + 5]
        own_ref, oth_ref, dug_out, duu_out, zt_out = refs[nd + 5 : nd + 10]
        lhs, ugs, uus, dug, duu, zt, gs, lsem, usem, osem = refs[nd + 10 :]
        i = pl.program_id(0)
        me = lax.axis_index("tp")

        def lhs_copies():
            off, out = 0, []
            for j, d in enumerate(dy_refs):
                out.append(pltpu.make_async_copy(d, lhs.at[pl.ds(off, d.shape[0]), :], lsem.at[j]))
                off += d.shape[0]
            return out

        def u_copies():
            off, out = 0, []
            for j, (mask, first, rows) in enumerate(places):
                src = pl.ds(pl.multiple_of(jnp.bitwise_xor(me, mask) * shard + first, 64), rows)
                for k, (a, s) in enumerate(((ug_ref, ugs), (uu_ref, uus))):
                    dst = s.at[pl.ds(off, rows), pl.ds(0, f)]
                    out.append(pltpu.make_async_copy(a.at[src, :], dst, usem.at[k, j]))
                off += rows
            return out

        def out_copies():
            return [
                pltpu.make_async_copy(dug.at[:, pl.ds(0, f)], dug_out, osem.at[0]),
                pltpu.make_async_copy(duu.at[:, pl.ds(0, f)], duu_out, osem.at[1]),
                pltpu.make_async_copy(zt.at[pl.ds(0, f), :], zt_out, osem.at[2]),
            ]

        def epilogue(slot, col):
            cols = pl.ds(pl.multiple_of(col, bg), bg)
            for q in range(0, total, 128):
                r = pl.ds(q, 128)
                a32 = ugs[r, cols].astype(F32)
                u32 = uus[r, cols].astype(F32)
                s = 0.5 * jnp.tanh(0.5 * a32) + 0.5
                act = a32 * s
                g = gs[slot, r, :]
                duu[r, cols] = (g * act).astype(BF16)
                dug[r, cols] = (g * (u32 * s * (1.0 + a32 * (1.0 - s)))).astype(BF16)
                zt[cols, r] = (act * u32).astype(BF16).T

        @pl.when(i == 0)
        def _():
            for c in lhs_copies() + u_copies():
                c.start()
            for c in lhs_copies():
                c.wait()
            gs[0, :, pl.ds(0, rest)] = lax.dot_general(
                lhs[...], wd_ref[pl.ds(0, rest), :], NT, preferred_element_type=F32
            )
            for c in u_copies():
                c.wait()

        @pl.when((i > 0) & (i <= gsteps))
        def _():
            gs[lax.rem(i, 2)] = lax.dot_general(lhs[...], wd_ref[...], NT, preferred_element_type=F32)
            epilogue(lax.rem(i + 1, 2), jnp.where(i == 1, gsteps, i - 2) * bg)

        @pl.when(i == gsteps)
        def _():
            epilogue(gsteps % 2, (gsteps - 1) * bg)
            for c in out_copies():
                c.start()

        @pl.when(i > gsteps)
        def _():
            acc = lax.dot_general(dug[:, pl.ds(0, f)], wg_ref[...], NT, preferred_element_type=F32)
            acc += lax.dot_general(duu[:, pl.ds(0, f)], wu_ref[...], NT, preferred_element_type=F32)
            own_ref[...] = acc[:half].astype(BF16)
            oth_ref[...] = acc[half:].astype(BF16)

        @pl.when(i == gsteps + psteps)
        def _():
            for c in out_copies():
                c.wait()

    wd_block = lambda i: (jnp.where(i == 0, gsteps, jnp.minimum(i, gsteps) - 1), 0)
    p_block = lambda i: jnp.maximum(i - gsteps - 1, 0)
    return pl.pallas_call(
        kernel,
        grid=(gsteps + 1 + psteps,),
        in_specs=[ANY] * nd
        + [pl.BlockSpec((bg, h), wd_block), ANY, ANY]
        + [pl.BlockSpec((bp, f), lambda i: (p_block(i), 0))] * 2,
        out_specs=[pl.BlockSpec((half, bp), lambda i: (0, p_block(i)))] * 2 + [ANY] * 3,
        scratch_shapes=[
            pltpu.VMEM((total, h), BF16),
            pltpu.VMEM((total, wide), BF16),
            pltpu.VMEM((total, wide), BF16),
            pltpu.VMEM((total, wide), BF16),
            pltpu.VMEM((total, wide), BF16),
            pltpu.VMEM((wide, total), BF16),
            pltpu.VMEM((2, total, bg), F32),
            pltpu.SemaphoreType.DMA((nd,)),
            pltpu.SemaphoreType.DMA((2, npc)),
            pltpu.SemaphoreType.DMA((3,)),
        ],
        out_shape=[
            jax.ShapeDtypeStruct((half, h), BF16),
            jax.ShapeDtypeStruct((half, h), BF16),
            jax.ShapeDtypeStruct((total, f), BF16),
            jax.ShapeDtypeStruct((total, f), BF16),
            jax.ShapeDtypeStruct((f, total), BF16),
        ],
        compiler_params=params(),
        cost_estimate=cost(total, 3 * h, f, 2 * (3 * f * h + total * (2 * h + 5 * f))),
        name="gp_chunk",
    )(*dys, wd, ug, uu, wg, wu)


def dw(streamed, moves, resident, transposed):
    ns, nr = len(streamed), len(resident)
    nm = len(moves)
    h = streamed[0].shape[1]
    if transposed:
        tokens, f = sum(r.shape[0] for r in resident), resident[0].shape[1]
        res_shape = (tokens, f)
    else:
        tokens, f = sum(r.shape[1] for r in resident), resident[0].shape[0]
        res_shape = (f, tokens)
    bn = 512
    steps = h // bn

    def kernel(*refs):
        s_refs = refs[:ns]
        r_refs = refs[ns : ns + nr]
        out_ref, buf, res, sem, rsem = refs[ns + nr :]
        i = pl.program_id(0)
        slot = lax.rem(i, 2)

        def block(step, where):
            cols = pl.ds(pl.multiple_of(step * bn, bn), bn)
            return [
                pltpu.make_async_copy(
                    s_refs[a].at[pl.ds(src, n), cols], buf.at[where, pl.ds(dst, n), :], sem.at[where, m]
                )
                for m, (a, src, n, dst) in enumerate(moves)
            ]

        @pl.when(i == 0)
        def _():
            for c in block(0, 0):
                c.start()
            copies, off = [], 0
            for j, r in enumerate(r_refs):
                n = r.shape[0] if transposed else r.shape[1]
                dst = res.at[pl.ds(off, n), :] if transposed else res.at[:, pl.ds(off, n)]
                c = pltpu.make_async_copy(r, dst, rsem.at[j])
                c.start()
                copies.append(c)
                off += n
            for c in copies:
                c.wait()

        @pl.when(i + 1 < steps)
        def _():
            for c in block(i + 1, lax.rem(i + 1, 2)):
                c.start()

        for c in block(i, slot):
            c.wait()
        if transposed:
            out_ref[...] = lax.dot_general(buf[slot], res[...], TN, preferred_element_type=F32)
        else:
            out_ref[...] = jnp.dot(res[...], buf[slot], preferred_element_type=F32)

    if transposed:
        out_spec, out_shape = pl.BlockSpec((bn, f), lambda i: (i, 0)), (h, f)
    else:
        out_spec, out_shape = pl.BlockSpec((f, bn), lambda i: (0, i)), (f, h)
    return pl.pallas_call(
        kernel,
        grid=(steps,),
        in_specs=[ANY] * (ns + nr),
        out_specs=out_spec,
        out_shape=jax.ShapeDtypeStruct(out_shape, F32),
        scratch_shapes=[
            pltpu.VMEM((2, tokens, bn), BF16),
            pltpu.VMEM(res_shape, BF16),
            pltpu.SemaphoreType.DMA((2, nm)),
            pltpu.SemaphoreType.DMA((nr,)),
        ],
        compiler_params=params(),
        cost_estimate=cost(tokens, h, f, 2 * tokens * (h + f) + 4 * h * f),
        name="dw",
    )(*streamed, *resident)


def solution(mesh):
    tok = P(("dp", "tp"), None)
    col = P(None, "tp")
    row = P("tp", None)
    act = P("dp", "tp")
    n = mesh.shape["tp"]
    pairs = {m: [(i, i ^ m) for i in range(n)] for m in (1, 2, 4)}
    core, xn, yn = pairs[1], pairs[2], pairs[4]

    def send(a, to):
        return lax.ppermute(a, "tp", to)

    def add(*terms):
        return functools.reduce(lambda a, b: a + b, [t.astype(F32) for t in terms]).astype(BF16)

    def inner(x, dy, wg, wu, wd, ug, uu):
        t = x.shape[0]
        u = t // 2
        dyp = [dy[:u], dy[u:]]
        dyc = send(dy, core)
        dyx0 = send(dyp[0], xn)
        dyy1 = send(dyp[1], yn)
        dyx1 = send(dyp[1], xn)
        dyy0 = send(dyp[0], yn)
        dyxc0, dyyc1 = send(dyx0, core), send(dyy1, core)
        dyd0, dyd1 = send(dyx0, yn), send(dyy1, xn)
        dyxc1, dyyc0 = send(dyx1, core), send(dyy0, core)
        dydc0, dydc1 = send(dyd0, core), send(dyd1, core)
        xx, xy, xc = send(x, xn), send(x, yn), send(x, core)
        xd0, xd1 = send(xx[:u], yn), send(xy[u:], xn)
        xxc, xyc = send(xx, core), send(xy, core)
        xdc0, xdc1 = send(xd0, core), send(xd1, core)

        chunks = (
            ([dy, dyc], [(0, 0, t), (1, 0, t)]),
            ([dyx0, dyy1, dyxc0, dyyc1], [(2, 0, u), (4, u, u), (3, 0, u), (5, u, u)]),
            ([dyx1, dyy0, dyxc1, dyyc0], [(2, u, u), (4, 0, u), (3, u, u), (5, 0, u)]),
            ([dyd0, dyd1, dydc0, dydc1], [(6, 0, t), (7, 0, t)]),
        )
        own, oth, dug, duu, zt = [], [], [], [], []
        for rows, places in chunks:
            res = gp_chunk(rows, wd, ug, uu, wg, wu, places)
            for dst, r in zip((own, oth, dug, duu, zt), res):
                dst.append(r)
        got = [send(oth[c], core) for c in range(4)]
        mine = lambda c, j: (own[c][j * u : (j + 1) * u], got[c][j * u : (j + 1) * u])
        rdx = send(add(*mine(3, 0)), xn)
        rdy = send(add(*mine(3, 1)), yn)
        rx0 = send(add(*mine(1, 0)), xn)
        ry1 = send(add(*mine(1, 1)), yn)
        rx1 = send(add(*mine(2, 0), rdy), xn)
        ry0 = send(add(*mine(2, 1), rdx), yn)
        dx = jnp.concatenate([add(*mine(0, 0), rx0, ry0), add(*mine(0, 1), rx1, ry1)])

        def moves(parts):
            out, dst = [], 0
            for a, src, rows in parts:
                out.append((a, src, rows, dst))
                dst += rows
            return out

        dy_arrays = [a for rows, _ in chunks for a in rows]
        dy_moves = moves([(k, 0, a.shape[0]) for k, a in enumerate(dy_arrays)])
        dwd = dw(dy_arrays, dy_moves, zt, False)
        x_arrays = [x, xc, xx, xy, xxc, xyc, xd0, xd1, xdc0, xdc1]
        x_moves = moves(
            [(0, 0, t), (1, 0, t), (2, 0, u), (3, u, u), (4, 0, u), (5, u, u), (2, u, u), (3, 0, u), (4, u, u), (5, 0, u)]
            + [(k, 0, u) for k in (6, 7, 8, 9)]
        )
        dwg = dw(x_arrays, x_moves, dug, True)
        dwu = dw(x_arrays, x_moves, duu, True)
        return dx, dwg, dwu, dwd

    return jax.shard_map(
        inner, mesh=mesh, in_specs=(tok, tok, col, col, row, act, act), out_specs=(tok, act, act, tok), check_vma=False
    )
```

```python
import functools

import jax
import jax.numpy as jnp
from jax import lax
from jax.experimental import pallas as pl
from jax.experimental.pallas import tpu as pltpu
from jax.sharding import PartitionSpec as P


BF16 = jnp.bfloat16
F32 = jnp.float32
VMEM_LIMIT = 60 * 1024 * 1024
SPLIT = 1
DWD_BLOCK = 256
ANY = pl.BlockSpec(memory_space=pl.ANY)
NT = (((1,), (1,)), ((), ()))
TN = (((0,), (0,)), ((), ()))


def params():
    return pltpu.CompilerParams(vmem_limit_bytes=VMEM_LIMIT)


def cost(m, k, n, nbytes):
    return pl.CostEstimate(flops=2 * m * k * n, bytes_accessed=nbytes, transcendentals=0)


def gp_chunk(dys, wd, ug, uu, wg, wu, places):
    f, h = wd.shape
    total = sum(d.shape[0] for d in dys)
    shard = ug.shape[0] // 8
    half = total // 2
    bg, bp = 512, 512
    gsteps, psteps = f // bg, h // bp
    rest = f - gsteps * bg
    nd, npc = len(dys), len(places)
    part = total // SPLIT
    nk = 4
    kb = h // nk

    def kernel(*refs):
        dy_refs = refs[:nd]
        wd_ref, ug_ref, uu_ref, wg_ref, wu_ref = refs[nd : nd + 5]
        own_ref, oth_ref, dug_out, duu_out, zt_out = refs[nd + 5 : nd + 10]
        lhs, wdb, ugs, uus, du, zt, gs, wbuf, lsem, dsem, ksem, usem, osem, wsem = refs[nd + 10 :]
        i = pl.program_id(0)
        me = lax.axis_index("tp")

        def lhs_copies(k):
            off, out = 0, []
            cols = pl.ds(k * kb, kb)
            for j, d in enumerate(dy_refs):
                out.append(pltpu.make_async_copy(d.at[:, cols], lhs.at[pl.ds(off, d.shape[0]), cols], lsem.at[k, j]))
                off += d.shape[0]
            out.append(pltpu.make_async_copy(wd_ref.at[pl.ds(0, bg), cols], wdb.at[0, :, cols], ksem.at[k]))
            return out

        def wd_copy(b):
            n = bg if b < gsteps else rest
            return pltpu.make_async_copy(
                wd_ref.at[pl.ds(b * bg, n), :], wdb.at[b % 2, pl.ds(0, n), :], dsem.at[b]
            )

        def u_copies(b):
            off, out = 0, []
            cols = pl.ds(b * bg, bg if b < gsteps else rest)
            for j, (mask, first, rows) in enumerate(places):
                src = pl.ds(pl.multiple_of(jnp.bitwise_xor(me, mask) * shard + first, 64), rows)
                for k, (a, s) in enumerate(((ug_ref, ugs), (uu_ref, uus))):
                    out.append(
                        pltpu.make_async_copy(a.at[src, cols], s.at[pl.ds(off, rows), cols], usem.at[b, k, j])
                    )
                off += rows
            return out

        def out_copy(k):
            src = (du.at[:, pl.ds(0, f)], du.at[:, pl.ds(f, f)], zt)[k]
            return pltpu.make_async_copy(src, (dug_out, duu_out, zt_out)[k], osem.at[k])

        def w_copies(step, slot):
            rows = pl.ds(pl.multiple_of(step * bp, bp), bp)
            return [
                pltpu.make_async_copy(w.at[rows, :], wbuf.at[slot, :, pl.ds(k * f, f)], wsem.at[slot, k])
                for k, w in enumerate((wg_ref, wu_ref))
            ]

        def start(copies):
            for c in copies:
                c.start()

        def wait(copies):
            for c in copies:
                c.wait()

        def epilogue(col, wide, first, rows):
            cols = pl.ds(pl.multiple_of(col, 256), wide)
            cols2 = pl.ds(pl.multiple_of(col + f, 256), wide)
            for q in range(0, rows, 128):
                r = pl.ds(pl.multiple_of(first + q, 128), 128)
                a32 = ugs[r, cols].astype(F32)
                u32 = uus[r, cols].astype(F32)
                s = 0.5 * jnp.tanh(0.5 * a32) + 0.5
                act = a32 * s
                g = gs[r, pl.ds(0, wide)]
                du[r, cols] = (g * (u32 * s * (1.0 + a32 * (1.0 - s)))).astype(BF16)
                du[r, cols2] = (g * act).astype(BF16)
                zt[cols, r] = (act * u32).astype(BF16).T

        @pl.when(i == 0)
        def _():
            for k in range(nk):
                start(lhs_copies(k))
            start([wd_copy(1)] + u_copies(0))

            def quarter(k, carry):
                for j in range(nk):

                    @pl.when(k == j)
                    def _():
                        wait(lhs_copies(j))

                cols = pl.ds(pl.multiple_of(k * kb, kb), kb)
                g = lax.dot_general(lhs[:, cols], wdb[0, :, cols], NT, preferred_element_type=F32)
                gs[...] = gs[...] + g
                return carry

            gs[...] = jnp.zeros_like(gs)
            lax.fori_loop(0, nk, quarter, 0)

        for b in range(1, gsteps):

            @pl.when(i == b)
            def _():
                start([wd_copy(b + 1)] + u_copies(b))
                wait([wd_copy(b)] + u_copies(b - 1))

        @pl.when((i > 0) & (i < gsteps))
        def _():
            def rows_of(j, carry):
                first = pl.multiple_of(j * part, 128)
                epilogue((i - 1) * bg, bg, first, part)
                r = pl.ds(first, part)
                gs[r, :] = lax.dot_general(lhs[r, :], wdb[lax.rem(i, 2)], NT, preferred_element_type=F32)
                return carry

            if SPLIT == 1:
                rows_of(0, 0)
            else:
                lax.fori_loop(0, SPLIT, rows_of, 0)

        @pl.when(i == gsteps)
        def _():
            start(u_copies(gsteps) + w_copies(0, 0) + w_copies(1, 1))
            wait([wd_copy(gsteps)] + u_copies(gsteps - 1))
            epilogue((gsteps - 1) * bg, bg, 0, total)
            gs[:, pl.ds(0, rest)] = lax.dot_general(
                lhs[...], wdb[gsteps % 2, pl.ds(0, rest), :], NT, preferred_element_type=F32
            )
            wait(u_copies(gsteps))

            def rows_of(j, carry):
                epilogue(gsteps * bg, rest, j * 128, 128)
                return carry

            lax.fori_loop(0, total // 128, rows_of, 0)

        @pl.when(i > gsteps)
        def _():
            step = i - gsteps - 1
            slot = lax.rem(step, 2)

            @pl.when((step > 0) & (step + 1 < psteps))
            def _():
                start(w_copies(step + 1, 1 - slot))

            for k in range(3):

                @pl.when(step == k + 1)
                def _():
                    out_copy(k).start()

            wait(w_copies(step, slot))
            acc = lax.dot_general(du[...], wbuf[slot], NT, preferred_element_type=F32)
            own_ref[...] = acc[:half].astype(BF16)
            oth_ref[...] = acc[half:].astype(BF16)

        @pl.when(i == gsteps + psteps)
        def _():
            wait([out_copy(k) for k in range(3)])

    p_block = lambda i: jnp.maximum(i - gsteps - 1, 0)
    return pl.pallas_call(
        kernel,
        grid=(gsteps + 1 + psteps,),
        in_specs=[ANY] * (nd + 5),
        out_specs=[pl.BlockSpec((half, bp), lambda i: (0, p_block(i)))] * 2 + [ANY] * 3,
        scratch_shapes=[
            pltpu.VMEM((total, h), BF16),
            pltpu.VMEM((2, bg, h), BF16),
            pltpu.VMEM((total, f), BF16),
            pltpu.VMEM((total, f), BF16),
            pltpu.VMEM((total, 2 * f), BF16),
            pltpu.VMEM((f, total), BF16),
            pltpu.VMEM((total, bg), F32),
            pltpu.VMEM((2, bp, 2 * f), BF16),
            pltpu.SemaphoreType.DMA((nk, nd)),
            pltpu.SemaphoreType.DMA((gsteps + 1,)),
            pltpu.SemaphoreType.DMA((nk,)),
            pltpu.SemaphoreType.DMA((gsteps + 1, 2, npc)),
            pltpu.SemaphoreType.DMA((3,)),
            pltpu.SemaphoreType.DMA((2, 2)),
        ],
        out_shape=[
            jax.ShapeDtypeStruct((half, h), BF16),
            jax.ShapeDtypeStruct((half, h), BF16),
            jax.ShapeDtypeStruct((total, f), BF16),
            jax.ShapeDtypeStruct((total, f), BF16),
            jax.ShapeDtypeStruct((f, total), BF16),
        ],
        compiler_params=params(),
        cost_estimate=cost(total, 3 * h, f, 2 * (3 * f * h + total * (2 * h + 5 * f))),
        name="gp_chunk",
    )(*dys, wd, ug, uu, wg, wu)


def dw(streamed, moves, resident, transposed, bn):
    ns, nm, nc = len(streamed), len(moves), len(resident[0])
    nr = len(resident) * nc
    h = streamed[0].shape[1]
    if transposed:
        rows, f = resident[0][0].shape
        res_shape = (rows * nc, len(resident) * f)
        out_block, out_map, out_shape = (bn, f), lambda i: (i, 0), (h, f)
    else:
        f, rows = resident[0][0].shape
        res_shape = (f, rows * nc)
        out_block, out_map, out_shape = (f, bn), lambda i: (0, i), (f, h)
    tokens, nout = rows * nc, len(resident)
    steps = h // bn

    def kernel(*refs):
        s_refs = refs[:ns]
        r_refs = refs[ns : ns + nr]
        outs = refs[ns + nr : ns + nr + nout]
        buf, res, sem, rsem = refs[ns + nr + nout :]
        i = pl.program_id(0)
        slot = lax.rem(i, 2)

        def block(step, where):
            cols = pl.ds(pl.multiple_of(step * bn, bn), bn)
            return [
                pltpu.make_async_copy(
                    s_refs[a].at[pl.ds(src, n), cols], buf.at[where, pl.ds(dst, n), :], sem.at[where, m]
                )
                for m, (a, src, n, dst) in enumerate(moves)
            ]

        def chunk(c):
            out = []
            for k in range(nout):
                toks = pl.ds(c * rows, rows)
                dst = res.at[toks, pl.ds(k * f, f)] if transposed else res.at[:, toks]
                out.append(pltpu.make_async_copy(r_refs[k * nc + c], dst, rsem.at[k, c]))
            return out

        def dot(where, toks):
            s = buf[where, toks, :]
            if transposed:
                return lax.dot_general(s, res[toks, :], TN, preferred_element_type=F32)
            return jnp.dot(res[:, toks], s, preferred_element_type=F32)

        @pl.when(i == 0)
        def _():
            for c in block(0, 0):
                c.start()
            for c in range(nc):
                for d in chunk(c):
                    d.start()

        @pl.when(i + 1 < steps)
        def _():
            for c in block(i + 1, 1 - slot):
                c.start()

        for c in block(i, slot):
            c.wait()

        @pl.when(i == 0)
        def _():
            for o in outs:
                o[...] = jnp.zeros_like(o)

            def add_chunk(c, carry):
                for j in range(nc):

                    @pl.when(c == j)
                    def _():
                        for d in chunk(j):
                            d.wait()

                toks = pl.ds(pl.multiple_of(c * rows, rows), rows)
                p = dot(0, toks)
                for k, o in enumerate(outs):
                    o[...] += p[:, k * f : (k + 1) * f] if transposed else p
                return carry

            lax.fori_loop(0, nc, add_chunk, 0)

        @pl.when(i > 0)
        def _():
            p = dot(slot, pl.ds(0, tokens))
            for k, o in enumerate(outs):
                o[...] = p[:, k * f : (k + 1) * f] if transposed else p

    return pl.pallas_call(
        kernel,
        grid=(steps,),
        in_specs=[ANY] * (ns + nr),
        out_specs=[pl.BlockSpec(out_block, out_map)] * nout,
        out_shape=[jax.ShapeDtypeStruct(out_shape, F32)] * nout,
        scratch_shapes=[
            pltpu.VMEM((2, tokens, bn), BF16),
            pltpu.VMEM(res_shape, BF16),
            pltpu.SemaphoreType.DMA((2, nm)),
            pltpu.SemaphoreType.DMA((nout, nc)),
        ],
        compiler_params=params(),
        cost_estimate=cost(tokens, h, nout * f, 2 * tokens * (h + nout * f) + 4 * nout * h * f),
        name="dw",
    )(*streamed, *[r for group in resident for r in group])


def dx_sum(base, rx, ry):
    t, h = base.shape
    bc = h // 2
    u = t // 2

    def kernel(base_ref, rx0, rx1, ry0, ry1, out_ref):
        for k, (a, b) in enumerate(((rx0, ry0), (rx1, ry1))):

            @pl.when(pl.program_id(0) == k)
            def _():
                total = base_ref[...].astype(F32) + a[...].astype(F32) + b[...].astype(F32)
                out_ref[...] = total.astype(BF16)

    first = pl.BlockSpec((u, bc), lambda i, j: (0, jnp.where(i == 0, j, 1)))
    second = pl.BlockSpec((u, bc), lambda i, j: (0, jnp.where(i == 1, j, 0)))
    both = pl.BlockSpec((u, bc), lambda i, j: (i, j))
    return pl.pallas_call(
        kernel,
        grid=(2, 2),
        in_specs=[both, first, second, first, second],
        out_specs=both,
        out_shape=jax.ShapeDtypeStruct((t, h), BF16),
        compiler_params=params(),
        cost_estimate=cost(t, 2, h, 8 * t * h),
        name="dx_sum",
    )(base, *rx, *ry)


def solution(mesh):
    tok = P(("dp", "tp"), None)
    col = P(None, "tp")
    row = P("tp", None)
    act = P("dp", "tp")
    n = mesh.shape["tp"]
    pairs = {m: [(i, i ^ m) for i in range(n)] for m in (1, 2, 4)}
    core, xn, yn = pairs[1], pairs[2], pairs[4]

    def send(a, to):
        return lax.ppermute(a, "tp", to)

    def add(*terms):
        return functools.reduce(lambda a, b: a + b, [t.astype(F32) for t in terms]).astype(BF16)

    def inner(x, dy, wg, wu, wd, ug, uu):
        t = x.shape[0]
        u = t // 2
        dyp = [dy[:u], dy[u:]]
        dyc = send(dy, core)
        dyx0 = send(dyp[0], xn)
        dyy1 = send(dyp[1], yn)
        dyx1 = send(dyp[1], xn)
        dyy0 = send(dyp[0], yn)
        dyxc0, dyyc1 = send(dyx0, core), send(dyy1, core)
        dyd0, dyd1 = send(dyx0, yn), send(dyy1, xn)
        dyxc1, dyyc0 = send(dyx1, core), send(dyy0, core)
        dydc0, dydc1 = send(dyd0, core), send(dyd1, core)
        xp = [x[:u], x[u:]]
        xc = send(x, core)
        xx0, xy1 = send(xp[0], xn), send(xp[1], yn)
        xx1, xy0 = send(xp[1], xn), send(xp[0], yn)
        xd0, xd1 = send(xx0, yn), send(xy1, xn)
        xxc0, xyc1 = send(xx0, core), send(xy1, core)
        xxc1, xyc0 = send(xx1, core), send(xy0, core)
        xdc0, xdc1 = send(xd0, core), send(xd1, core)

        chunks = (
            ([dy, dyc], [(0, 0, t), (1, 0, t)]),
            ([dyx0, dyy1, dyxc0, dyyc1], [(2, 0, u), (4, u, u), (3, 0, u), (5, u, u)]),
            ([dyx1, dyy0, dyxc1, dyyc0], [(2, u, u), (4, 0, u), (3, u, u), (5, 0, u)]),
            ([dyd0, dyd1, dydc0, dydc1], [(6, 0, t), (7, 0, t)]),
        )
        own, oth, dug, duu, zt = [], [], [], [], []
        for rows, places in chunks:
            res = gp_chunk(rows, wd, ug, uu, wg, wu, places)
            for dst, r in zip((own, oth, dug, duu, zt), res):
                dst.append(r)
        got = [send(oth[c], core) for c in range(4)]
        mine = lambda c, j: (own[c][j * u : (j + 1) * u], got[c][j * u : (j + 1) * u])
        rdx = send(add(*mine(3, 0)), xn)
        rdy = send(add(*mine(3, 1)), yn)
        qx0, qy1 = add(*mine(1, 0)), add(*mine(1, 1))
        rx0, ry1 = send(qx0, xn), send(qy1, yn)
        rx1 = send(add(*mine(2, 0), rdy), xn)
        ry0 = send(add(*mine(2, 1), rdx), yn)
        base = add(own[0], got[0])
        dx = dx_sum(base, (rx0, rx1), (ry0, ry1))

        def moves(parts):
            out, dst = [], 0
            for a, src, rows in parts:
                out.append((a, src, rows, dst))
                dst += rows
            return out

        dy_arrays = [a for rows, _ in chunks for a in rows]
        dy_moves = moves([(k, 0, a.shape[0]) for k, a in enumerate(dy_arrays)])
        (dwd,) = dw(dy_arrays, dy_moves, [zt], False, DWD_BLOCK)
        x_arrays = [x, xc, xx0, xy1, xxc0, xyc1, xx1, xy0, xxc1, xyc0, xd0, xd1, xdc0, xdc1]
        x_moves = moves([(k, 0, a.shape[0]) for k, a in enumerate(x_arrays)])
        dwg, dwu = dw(x_arrays, x_moves, [dug, duu], True, 256)
        return dx, dwg, dwu, dwd

    return jax.shard_map(
        inner, mesh=mesh, in_specs=(tok, tok, col, col, row, act, act), out_specs=(tok, act, act, tok), check_vma=False
    )
```

```python
import functools

import jax
import jax.numpy as jnp
from jax import lax
from jax.experimental import pallas as pl
from jax.experimental.pallas import tpu as pltpu
from jax.sharding import PartitionSpec as P


BF16 = jnp.bfloat16
F32 = jnp.float32
VMEM_LIMIT = 60 * 1024 * 1024
SPLIT = 1
DWD_BLOCK = 512
ANY = pl.BlockSpec(memory_space=pl.ANY)
NT = (((1,), (1,)), ((), ()))
TN = (((0,), (0,)), ((), ()))


def params():
    return pltpu.CompilerParams(vmem_limit_bytes=VMEM_LIMIT)


def cost(m, k, n, nbytes):
    return pl.CostEstimate(flops=2 * m * k * n, bytes_accessed=nbytes, transcendentals=0)


def gp_chunk(dys, wd, ug, uu, wg, wu, places, whole=None):
    f, h = wd.shape
    total = sum(d.shape[0] for d in dys)
    shard = ug.shape[0] // 8
    half = total // 2
    bg, bp = 512, 512
    gsteps, psteps = f // bg, h // bp
    rest = f - gsteps * bg
    nd, npc = len(dys), len(places)
    part = total // SPLIT
    nk = 4
    kb = h // nk
    nw = 0 if whole is None else 1

    def kernel(*refs):
        dy_refs = refs[:nd]
        wd_ref, ug_ref, uu_ref, wg_ref, wu_ref = refs[nd : nd + 5]
        outs = refs[nd + 5 + nw :]
        own_ref, oth_ref, dug_out, duu_out, zt_out = outs[:5]
        lhs, wdb, ugs, uus, du, zt, gs, wbuf, lsem, dsem, ksem, usem, osem, wsem = outs[5 + 2 * nw : 19 + 2 * nw]
        i = pl.program_id(0)
        me = lax.axis_index("tp")

        def lhs_copies(k):
            off, out = 0, []
            cols = pl.ds(k * kb, kb)
            for j, d in enumerate(dy_refs):
                out.append(pltpu.make_async_copy(d.at[:, cols], lhs.at[pl.ds(off, d.shape[0]), cols], lsem.at[k, j]))
                off += d.shape[0]
            out.append(pltpu.make_async_copy(wd_ref.at[pl.ds(0, bg), cols], wdb.at[0, :, cols], ksem.at[k]))
            return out

        def wd_copy(b):
            n = bg if b < gsteps else rest
            return pltpu.make_async_copy(
                wd_ref.at[pl.ds(b * bg, n), :], wdb.at[b % 2, pl.ds(0, n), :], dsem.at[b]
            )

        def u_copies(b):
            off, out = 0, []
            cols = pl.ds(b * bg, bg if b < gsteps else rest)
            for j, (mask, first, rows) in enumerate(places):
                src = pl.ds(pl.multiple_of(jnp.bitwise_xor(me, mask) * shard + first, 64), rows)
                for k, (a, s) in enumerate(((ug_ref, ugs), (uu_ref, uus))):
                    out.append(
                        pltpu.make_async_copy(a.at[src, cols], s.at[pl.ds(off, rows), cols], usem.at[b, k, j])
                    )
                off += rows
            return out

        def out_copy(k):
            src = (du.at[:, pl.ds(0, f)], du.at[:, pl.ds(f, f)], zt)[k]
            return pltpu.make_async_copy(src, (dug_out, duu_out, zt_out)[k], osem.at[k])

        def half_in(k):
            r = pl.ds(k * (whole.shape[0] // 2), whole.shape[0] // 2)
            return pltpu.make_async_copy(refs[nd + 5].at[r, :], outs[-2].at[r, :], outs[-1].at[k])

        def half_out(k):
            r = pl.ds(k * (whole.shape[0] // 2), whole.shape[0] // 2)
            return pltpu.make_async_copy(outs[-2].at[r, :], outs[5 + k], outs[-1].at[2 + k])

        def w_copies(step, slot):
            rows = pl.ds(pl.multiple_of(step * bp, bp), bp)
            return [
                pltpu.make_async_copy(w.at[rows, :], wbuf.at[slot, :, pl.ds(k * f, f)], wsem.at[slot, k])
                for k, w in enumerate((wg_ref, wu_ref))
            ]

        def start(copies):
            for c in copies:
                c.start()

        def wait(copies):
            for c in copies:
                c.wait()

        def epilogue(col, wide, first, rows):
            cols = pl.ds(pl.multiple_of(col, 256), wide)
            cols2 = pl.ds(pl.multiple_of(col + f, 256), wide)
            for q in range(0, rows, 128):
                r = pl.ds(pl.multiple_of(first + q, 128), 128)
                a32 = ugs[r, cols].astype(F32)
                u32 = uus[r, cols].astype(F32)
                s = 0.5 * jnp.tanh(0.5 * a32) + 0.5
                act = a32 * s
                g = gs[r, pl.ds(0, wide)]
                du[r, cols] = (g * (u32 * s * (1.0 + a32 * (1.0 - s)))).astype(BF16)
                du[r, cols2] = (g * act).astype(BF16)
                zt[cols, r] = (act * u32).astype(BF16).T

        @pl.when(i == 0)
        def _():
            for k in range(nk):
                start(lhs_copies(k))
            start([wd_copy(1)] + u_copies(0))

            def quarter(k, carry):
                for j in range(nk):

                    @pl.when(k == j)
                    def _():
                        wait(lhs_copies(j))

                cols = pl.ds(pl.multiple_of(k * kb, kb), kb)
                g = lax.dot_general(lhs[:, cols], wdb[0, :, cols], NT, preferred_element_type=F32)
                gs[...] = gs[...] + g
                return carry

            gs[...] = jnp.zeros_like(gs)
            lax.fori_loop(0, nk, quarter, 0)

        for b in range(1, gsteps):

            @pl.when(i == b)
            def _():
                start([wd_copy(b + 1)] + u_copies(b))
                wait([wd_copy(b)] + u_copies(b - 1))

        @pl.when((i > 0) & (i < gsteps))
        def _():
            def rows_of(j, carry):
                first = pl.multiple_of(j * part, 128)
                epilogue((i - 1) * bg, bg, first, part)
                r = pl.ds(first, part)
                gs[r, :] = lax.dot_general(lhs[r, :], wdb[lax.rem(i, 2)], NT, preferred_element_type=F32)
                return carry

            if SPLIT == 1:
                rows_of(0, 0)
            else:
                lax.fori_loop(0, SPLIT, rows_of, 0)

        @pl.when(i == gsteps)
        def _():
            start(u_copies(gsteps) + w_copies(0, 0) + w_copies(1, 1))
            wait([wd_copy(gsteps)] + u_copies(gsteps - 1))
            epilogue((gsteps - 1) * bg, bg, 0, total)
            gs[:, pl.ds(0, rest)] = lax.dot_general(
                lhs[...], wdb[gsteps % 2, pl.ds(0, rest), :], NT, preferred_element_type=F32
            )
            wait(u_copies(gsteps))

            def rows_of(j, carry):
                epilogue(gsteps * bg, rest, j * 128, 128)
                return carry

            lax.fori_loop(0, total // 128, rows_of, 0)

        @pl.when(i > gsteps)
        def _():
            step = i - gsteps - 1
            slot = lax.rem(step, 2)

            @pl.when((step > 0) & (step + 1 < psteps))
            def _():
                start(w_copies(step + 1, 1 - slot))

            for k in range(3):

                @pl.when(step == k + 1)
                def _():
                    out_copy(k).start()

            if nw:

                @pl.when(step == 4)
                def _():
                    start([half_in(k) for k in range(2)])

                @pl.when(step == 7)
                def _():
                    wait([half_in(k) for k in range(2)])
                    start([half_out(k) for k in range(2)])

            wait(w_copies(step, slot))
            acc = lax.dot_general(du[...], wbuf[slot], NT, preferred_element_type=F32)
            own_ref[...] = acc[:half].astype(BF16)
            oth_ref[...] = acc[half:].astype(BF16)

        @pl.when(i == gsteps + psteps)
        def _():
            wait([out_copy(k) for k in range(3)])
            if nw:
                wait([half_out(k) for k in range(2)])

    p_block = lambda i: jnp.maximum(i - gsteps - 1, 0)
    return pl.pallas_call(
        kernel,
        grid=(gsteps + 1 + psteps,),
        in_specs=[ANY] * (nd + 5 + nw),
        out_specs=[pl.BlockSpec((half, bp), lambda i: (0, p_block(i)))] * 2 + [ANY] * (3 + 2 * nw),
        scratch_shapes=[
            pltpu.VMEM((total, h), BF16),
            pltpu.VMEM((2, bg, h), BF16),
            pltpu.VMEM((total, f), BF16),
            pltpu.VMEM((total, f), BF16),
            pltpu.VMEM((total, 2 * f), BF16),
            pltpu.VMEM((f, total), BF16),
            pltpu.VMEM((total, bg), F32),
            pltpu.VMEM((2, bp, 2 * f), BF16),
            pltpu.SemaphoreType.DMA((nk, nd)),
            pltpu.SemaphoreType.DMA((gsteps + 1,)),
            pltpu.SemaphoreType.DMA((nk,)),
            pltpu.SemaphoreType.DMA((gsteps + 1, 2, npc)),
            pltpu.SemaphoreType.DMA((3,)),
            pltpu.SemaphoreType.DMA((2, 2)),
        ]
        + ([pltpu.VMEM(whole.shape, BF16), pltpu.SemaphoreType.DMA((4,))] if nw else []),
        out_shape=[
            jax.ShapeDtypeStruct((half, h), BF16),
            jax.ShapeDtypeStruct((half, h), BF16),
            jax.ShapeDtypeStruct((total, f), BF16),
            jax.ShapeDtypeStruct((total, f), BF16),
            jax.ShapeDtypeStruct((f, total), BF16),
        ]
        + [jax.ShapeDtypeStruct((whole.shape[0] // 2, whole.shape[1]), BF16) for _ in range(2 * nw)],
        compiler_params=params(),
        cost_estimate=cost(total, 3 * h, f, 2 * (3 * f * h + total * (2 * h + 5 * f))),
        name="gp_chunk",
    )(*dys, wd, ug, uu, wg, wu, *([whole] if nw else []))


def dw(streamed, moves, resident, transposed, bn):
    ns, nm, nc = len(streamed), len(moves), len(resident[0])
    nr = len(resident) * nc
    h = streamed[0].shape[1]
    if transposed:
        rows, f = resident[0][0].shape
        res_shape = (rows * nc, len(resident) * f)
        out_block, out_map, out_shape = (bn, f), lambda i: (i, 0), (h, f)
    else:
        f, rows = resident[0][0].shape
        res_shape = (f, rows * nc)
        out_block, out_map, out_shape = (f, bn), lambda i: (0, i), (f, h)
    tokens, nout = rows * nc, len(resident)
    steps = h // bn

    def kernel(*refs):
        s_refs = refs[:ns]
        r_refs = refs[ns : ns + nr]
        outs = refs[ns + nr : ns + nr + nout]
        buf, res, sem, rsem = refs[ns + nr + nout :]
        i = pl.program_id(0)
        slot = lax.rem(i, 2)

        def block(step, where):
            cols = pl.ds(pl.multiple_of(step * bn, bn), bn)
            return [
                pltpu.make_async_copy(
                    s_refs[a].at[pl.ds(src, n), cols], buf.at[where, pl.ds(dst, n), :], sem.at[where, m]
                )
                for m, (a, src, n, dst) in enumerate(moves)
            ]

        def chunk(c):
            out = []
            for k in range(nout):
                toks = pl.ds(c * rows, rows)
                dst = res.at[toks, pl.ds(k * f, f)] if transposed else res.at[:, toks]
                out.append(pltpu.make_async_copy(r_refs[k * nc + c], dst, rsem.at[k, c]))
            return out

        def dot(where, toks):
            s = buf[where, toks, :]
            if transposed:
                return lax.dot_general(s, res[toks, :], TN, preferred_element_type=F32)
            return jnp.dot(res[:, toks], s, preferred_element_type=F32)

        @pl.when(i == 0)
        def _():
            for c in block(0, 0):
                c.start()
            for c in range(nc):
                for d in chunk(c):
                    d.start()

        @pl.when(i + 1 < steps)
        def _():
            for c in block(i + 1, 1 - slot):
                c.start()

        for c in block(i, slot):
            c.wait()

        @pl.when(i == 0)
        def _():
            for o in outs:
                o[...] = jnp.zeros_like(o)

            def add_chunk(c, carry):
                for j in range(nc):

                    @pl.when(c == j)
                    def _():
                        for d in chunk(j):
                            d.wait()

                toks = pl.ds(pl.multiple_of(c * rows, rows), rows)
                p = dot(0, toks)
                for k, o in enumerate(outs):
                    o[...] += p[:, k * f : (k + 1) * f] if transposed else p
                return carry

            lax.fori_loop(0, nc, add_chunk, 0)

        @pl.when(i > 0)
        def _():
            p = dot(slot, pl.ds(0, tokens))
            for k, o in enumerate(outs):
                o[...] = p[:, k * f : (k + 1) * f] if transposed else p

    return pl.pallas_call(
        kernel,
        grid=(steps,),
        in_specs=[ANY] * (ns + nr),
        out_specs=[pl.BlockSpec(out_block, out_map)] * nout,
        out_shape=[jax.ShapeDtypeStruct(out_shape, F32)] * nout,
        scratch_shapes=[
            pltpu.VMEM((2, tokens, bn), BF16),
            pltpu.VMEM(res_shape, BF16),
            pltpu.SemaphoreType.DMA((2, nm)),
            pltpu.SemaphoreType.DMA((nout, nc)),
        ],
        compiler_params=params(),
        cost_estimate=cost(tokens, h, nout * f, 2 * tokens * (h + nout * f) + 4 * nout * h * f),
        name="dw",
    )(*streamed, *[r for group in resident for r in group])


def solution(mesh):
    tok = P(("dp", "tp"), None)
    col = P(None, "tp")
    row = P("tp", None)
    act = P("dp", "tp")
    n = mesh.shape["tp"]
    pairs = {m: [(i, i ^ m) for i in range(n)] for m in (1, 2, 4)}
    core, xn, yn = pairs[1], pairs[2], pairs[4]

    def send(a, to):
        return lax.ppermute(a, "tp", to)

    def add(*terms):
        return functools.reduce(lambda a, b: a + b, [t.astype(F32) for t in terms]).astype(BF16)

    def inner(x, dy, wg, wu, wd, ug, uu):
        t = x.shape[0]
        u = t // 2
        dyp = [dy[:u], dy[u:]]
        dyc = send(dy, core)
        dyx0 = send(dyp[0], xn)
        dyy1 = send(dyp[1], yn)
        dyx1 = send(dyp[1], xn)
        dyy0 = send(dyp[0], yn)
        dyxc0, dyyc1 = send(dyx0, core), send(dyy1, core)
        dyd0, dyd1 = send(dyx0, yn), send(dyy1, xn)
        dyxc1, dyyc0 = send(dyx1, core), send(dyy0, core)
        dydc0, dydc1 = send(dyd0, core), send(dyd1, core)
        *first, xa, xb = gp_chunk([dy, dyc], wd, ug, uu, wg, wu, [(0, 0, t), (1, 0, t)], whole=x)
        xp = [xa, xb]
        xc = send(x, core)
        xx0, xy1 = send(xp[0], xn), send(xp[1], yn)
        xx1, xy0 = send(xp[1], xn), send(xp[0], yn)
        xd0, xd1 = send(xx0, yn), send(xy1, xn)
        xxc0, xyc1 = send(xx0, core), send(xy1, core)
        xxc1, xyc0 = send(xx1, core), send(xy0, core)
        xdc0, xdc1 = send(xd0, core), send(xd1, core)

        chunks = (
            ([dy, dyc], [(0, 0, t), (1, 0, t)]),
            ([dyx0, dyy1, dyxc0, dyyc1], [(2, 0, u), (4, u, u), (3, 0, u), (5, u, u)]),
            ([dyx1, dyy0, dyxc1, dyyc0], [(2, u, u), (4, 0, u), (3, u, u), (5, 0, u)]),
            ([dyd0, dyd1, dydc0, dydc1], [(6, 0, t), (7, 0, t)]),
        )
        own, oth, dug, duu, zt = [], [], [], [], []
        for c, (rows, places) in enumerate(chunks):
            res = first
            if c:
                res = gp_chunk(rows, wd, ug, uu, wg, wu, places)
            for dst, r in zip((own, oth, dug, duu, zt), res):
                dst.append(r)
        got = [send(oth[c], core) for c in range(4)]
        mine = lambda c, j: (own[c][j * u : (j + 1) * u], got[c][j * u : (j + 1) * u])
        rdx = send(add(*mine(3, 0)), xn)
        rdy = send(add(*mine(3, 1)), yn)
        qx0, qy1 = add(*mine(1, 0)), add(*mine(1, 1))
        rx0, ry1 = send(qx0, xn), send(qy1, yn)
        rx1 = send(add(*mine(2, 0), rdy), xn)
        ry0 = send(add(*mine(2, 1), rdx), yn)
        base = add(own[0], got[0])
        dx = jnp.concatenate([add(base[:u], rx0, ry0), add(base[u:], rx1, ry1)])

        def moves(parts):
            out, dst = [], 0
            for a, src, rows in parts:
                out.append((a, src, rows, dst))
                dst += rows
            return out

        dy_arrays = [a for rows, _ in chunks for a in rows]
        dy_moves = moves([(k, 0, a.shape[0]) for k, a in enumerate(dy_arrays)])
        (dwd,) = dw(dy_arrays, dy_moves, [zt], False, DWD_BLOCK)
        x_arrays = [x, xc, xx0, xy1, xxc0, xyc1, xx1, xy0, xxc1, xyc0, xd0, xd1, xdc0, xdc1]
        x_moves = moves([(k, 0, a.shape[0]) for k, a in enumerate(x_arrays)])
        dwg, dwu = dw(x_arrays, x_moves, [dug, duu], True, 256)
        return dx, dwg, dwu, dwd

    return jax.shard_map(
        inner, mesh=mesh, in_specs=(tok, tok, col, col, row, act, act), out_specs=(tok, act, act, tok), check_vma=False
    )
```
